32 devices in a mesh: horiz: 8 (over y, x, core), lev: 4 (over z).
Axes of the slice: x: 2, y: 2, z: 4, core: 2. Of those that a mesh axis runs over, the one named last changes fastest.
Arguments:
- source_state: bfloat16 [5, 68, 32768], P(None, 'lev', 'horiz'), may hold values from -6 to 6
- intersection: int32 [40], P('horiz'), may hold values from 0 to 7, as said below
- index_map: int32 [40, 512], P('horiz'), may hold values from 0 to 4095
- blocks: bfloat16 [40, 512, 2048], P('horiz'), may hold values from -0.125 to 0.125
- bracket: int32 [127, 16384], P(None, ('horiz', 'lev')), may hold values from 0 to 66
- fraction: float32 [127, 16384], P(None, ('horiz', 'lev')), may hold values from 0 to 1
Outputs:
- target_state: bfloat16 [5, 127, 16384], P(None, None, ('horiz', 'lev'))
The draws below stay inside these ranges and needn't reach their ends.
Inputs may be any that keep to these rules, and one draw needn't show every extreme that they name: For every target group g, intersection[g * 5] to intersection[g * 5 + 4] are the groups g - 2 to g + 2 modulo 8, each once, in some order.
All inputs are finite; a program needn't handle non-finite values.
Results may differ from the reference program's by a relative error of at most 0.0049.
Values may be sent and summed in bfloat16 or wider, within the bound.
No kernel may reach another device: no remote copies, remote signals or barrier semaphores. Data moves between devices by JAX's collectives and lax.ppermute only.
A program may use at most 64 MiB of HBM per device.

```python
import jax
import jax.numpy as jnp
from jax import lax

F = 5
LEVELS_OUT = 127
R = 2
SRC_DEV = 4096
P_SIZE = 512
TGT_DEV = 2048
K = 5
GROUPS = 8
LEVELS_IN = 68
SRC_CELLS = 32768
TGT_CELLS = 16384
BLOCKS = 40


def draw_intersection(key, part):
    subkeys = jax.random.split(key, GROUPS)
    orders = jax.vmap(lambda subkey: jax.random.permutation(subkey, K))(subkeys)
    group_ids = jnp.arange(GROUPS, dtype=jnp.int32)[:, None]
    return ((group_ids + orders.astype(jnp.int32) - R) % GROUPS).reshape(-1).astype(jnp.int32)


def plant(drawn, key, least, high):
    extent = drawn.shape
    spot = [jax.random.randint(jax.random.fold_in(key, axis), (), 0, extent[axis]) for axis in range(len(extent))]
    drawn = drawn.at[tuple(spot)].set(least)
    longest = extent.index(max(extent))
    spot[longest] = (spot[longest] + 1) % extent[longest]
    return drawn.at[tuple(spot)].set(high)


def block_levels(key, extent, shards, smallest, top_value):
    def one(dim, parts):
        heights = jax.random.uniform(jax.random.fold_in(jax.random.fold_in(key, 6), dim), (parts,), jnp.float32, smallest / len(shards), top_value / len(shards))
        return jnp.repeat(jnp.exp(heights), extent[dim] // parts).reshape((-1,) + (1,) * (len(extent) - dim - 1))

    loudness = one(*shards[0])
    for cut in shards[1:]:
        loudness = loudness * one(*cut)
    return loudness


def scatter_about(key, dims, deviation, limit, pieces=(), held_as=jnp.bfloat16):
    array = jax.random.normal(key, dims, jnp.float32) * deviation
    if len(pieces) > 0:
        array = block_levels(key, dims, pieces, -0.22, 0.18) * array
    return jnp.clip(array, min=-limit, max=limit).astype(held_as)


def setup_inputs(seed: int = 0) -> dict:
    key_of = jax.random.split(jax.random.key(seed), 7)
    source_state = scatter_about(key_of[0], (F, LEVELS_IN, SRC_CELLS), 1.0, 6.0, ((1, 4), (2, 8)))
    intersection = draw_intersection(jax.random.fold_in(key_of[6], 71), 0)
    index_map = plant(jax.random.randint(key_of[2], (BLOCKS, P_SIZE), 0, SRC_DEV), jax.random.fold_in(key_of[2], 1), 0, SRC_DEV - 1).astype(jnp.int32)
    blocks = scatter_about(key_of[3], (BLOCKS, P_SIZE, TGT_DEV), (K * P_SIZE) ** -0.5, 0.125, ((0, 8),))
    bracket = plant(jax.random.randint(key_of[4], (LEVELS_OUT, TGT_CELLS), 0, LEVELS_IN - 1), jax.random.fold_in(key_of[4], 1), 0, (LEVELS_IN - 1) - 1).astype(jnp.int32)
    fraction = jnp.clip(1.0 * jax.random.uniform(key_of[5], (LEVELS_OUT, TGT_CELLS), jnp.float32) ** block_levels(key_of[5], (LEVELS_OUT, TGT_CELLS), ((1, 32),), -0.2, 0.2), 0.0, 1.0)
    return {"source_state": source_state, "intersection": intersection, "index_map": index_map, "blocks": blocks, "bracket": bracket, "fraction": fraction}


def reference(source_state, intersection, index_map, blocks, bracket, fraction):
    group_count = intersection.shape[0] // K
    fields_levels = F * LEVELS_IN
    source_tiles = jnp.transpose(source_state.reshape(fields_levels, group_count, SRC_DEV), (1, 0, 2))

    def remap_group(group_id):
        total_sum = jnp.zeros((fields_levels, TGT_DEV), jnp.float32)
        for block_slot in range(K):
            block_row = group_id * K + block_slot
            source_tile = source_tiles[intersection[block_row]]
            chosen = jnp.take(source_tile, index_map[block_row], axis=1).astype(jnp.float32)
            weights = blocks[block_row].astype(jnp.float32)
            total_sum = total_sum + jnp.dot(chosen, weights, preferred_element_type=jnp.float32)
        return total_sum.astype(jnp.bfloat16)

    remapped = lax.map(remap_group, jnp.arange(group_count, dtype=jnp.int32))
    horizontal = jnp.transpose(remapped, (1, 0, 2)).reshape(F, LEVELS_IN, group_count * TGT_DEV)
    widened = horizontal.astype(jnp.float32)
    below_level = jnp.take_along_axis(widened, bracket[None], axis=1)
    above_level = jnp.take_along_axis(widened, bracket[None] + 1, axis=1)
    upper_share = fraction[None]
    return ((1.0 - upper_share) * below_level + upper_share * above_level).astype(jnp.bfloat16)
```

```python
import jax
import jax.numpy as jnp
from jax import lax
from jax.experimental import pallas as pl
from jax.experimental.pallas import tpu as pltpu
from jax.sharding import PartitionSpec as P

SUB = 8
LANES = 128


def shifted(block, axis, distance):
    devices = range(lax.axis_size(axis))
    route = [((i - distance) % len(devices), i) for i in devices]
    return lax.ppermute(block, axis, route)


def select_cells(tile, wanted):
    cell_ids = jnp.arange(tile.shape[1], dtype=jnp.int32)[:, None]
    picker = (cell_ids == wanted[None, :]).astype(jnp.bfloat16)
    return jnp.dot(tile, picker, preferred_element_type=jnp.float32).astype(jnp.bfloat16)


def choose(values, bits):
    for bit in bits:
        pairs = [
            jnp.where(bit, values[i + 1], values[i]) if i + 1 < len(values) else values[i]
            for i in range(0, len(values), 2)
        ]
        values = pairs
    return values[0]


def interpolate_body(lower_ref, upper_ref, fraction_ref, *refs):
    slab_refs, out_ref, held_ref = refs[:-2], refs[-2], refs[-1]
    fields, levels_out, width = out_ref.shape
    slab = slab_refs[0].shape[0] // fields
    tiles = -(-len(slab_refs) * slab // SUB)
    for place, slab_ref in enumerate(slab_refs):
        rows = slab_ref[...].astype(jnp.float32)
        for f in range(fields):
            held_ref[f, place * slab : (place + 1) * slab, :] = rows[f * slab : (f + 1) * slab]
    digits = max(1, (tiles - 1).bit_length())
    step = 2 * SUB

    def load(ref, first, size, cols):
        value = ref[pl.ds(first, size), cols]
        if size < SUB:
            rest = jnp.zeros((SUB - size, LANES), value.dtype)
            value = jnp.concatenate([value, rest], axis=0)
        return value

    def split(row):
        tile = row >> 3
        return row & (SUB - 1), [(tile & (1 << i)) != 0 for i in range(digits)]

    def fetch(values, row):
        index, bits = row
        return choose(
            [jnp.take_along_axis(v, index, axis=0, mode="promise_in_bounds") for v in values], bits
        )

    def band(first, count, col):
        cols = pl.ds(col, LANES)
        halves = []
        for start in range(0, count, SUB):
            size = min(SUB, count - start)
            share = load(fraction_ref, first + start, size, cols)
            below = split(load(lower_ref, first + start, size, cols))
            above = split(load(upper_ref, first + start, size, cols))
            halves.append((below, above, share, 1.0 - share))
        for f in range(fields):
            values = [held_ref[f, k * SUB : (k + 1) * SUB, cols] for k in range(tiles)]
            results = [
                rest * fetch(values, below) + share * fetch(values, above)
                for below, above, share, rest in halves
            ]
            mixed = jnp.concatenate(results, axis=0)[:count]
            out_ref[f, pl.ds(first, count), cols] = mixed.astype(jnp.bfloat16)

    full = levels_out // step

    @pl.loop(0, width // LANES)
    def _(c):
        col = pl.multiple_of(c * LANES, LANES)

        @pl.loop(0, full)
        def _(j):
            band(pl.multiple_of(j * step, step), step, col)

        if levels_out % step:
            band(full * step, levels_out % step, col)


def interpolate(lower, upper, fraction, slabs, fields):
    rows, width = slabs[0].shape
    held = -(-len(slabs) * rows // fields // SUB) * SUB
    vmem = pl.BlockSpec(memory_space=pltpu.VMEM)
    return pl.pallas_call(
        interpolate_body,
        out_shape=jax.ShapeDtypeStruct((fields, lower.shape[0], width), jnp.bfloat16),
        in_specs=[vmem] * (3 + len(slabs)),
        out_specs=vmem,
        scratch_shapes=[pltpu.VMEM((fields, held, width), jnp.float32)],
        name="interpolate",
    )(lower, upper, fraction, *slabs)


def local(source_state, intersection, index_map, blocks, bracket, fraction):
    fields, level_slab, tile_cells = source_state.shape
    stacked = source_state.reshape(fields * level_slab, tile_cells)
    groups = lax.axis_size("horiz")
    block_count = intersection.shape[0]
    depth = (block_count - 1) // 2
    own_group = lax.axis_index("horiz")
    position = (intersection - own_group + depth) % groups
    collected = []
    for offset in range(-depth, depth + 1):
        wanted_group = (own_group + offset) % groups
        matched = intersection == wanted_group
        request = jnp.sum(jnp.where(matched[:, None], index_map, 0), axis=0)
        if offset == 0:
            collected.append(select_cells(stacked, request))
        else:
            incoming = shifted(request, "horiz", offset)
            outgoing = select_cells(stacked, incoming)
            collected.append(shifted(outgoing, "horiz", -offset))
    by_offset = jnp.stack(collected)
    pieces = [
        lax.dynamic_index_in_dim(by_offset, position[block_slot], 0, keepdims=False)
        for block_slot in range(block_count)
    ]
    chosen = jnp.concatenate(pieces, axis=1)
    weights_flat = blocks.reshape(-1, blocks.shape[2])
    horizontal = jnp.dot(chosen, weights_flat, preferred_element_type=jnp.float32).astype(
        jnp.bfloat16
    )
    shares = lax.axis_size("lev")
    own_share = lax.axis_index("lev")
    width = blocks.shape[2] // shares
    slabs = []
    for distance in range(shares):
        target = (own_share + distance) % shares
        part = lax.dynamic_slice_in_dim(horizontal, target * width, width, axis=1)
        slabs.append(part if distance == 0 else shifted(part, "lev", distance))

    def place(level):
        return (own_share - level // level_slab) % shares * level_slab + level % level_slab

    return interpolate(place(bracket), place(bracket + 1), fraction, slabs, fields)


def solution(mesh):
    in_specs = (
        P(None, "lev", "horiz"),
        P("horiz"),
        P("horiz", None),
        P("horiz", None, None),
        P(None, ("horiz", "lev")),
        P(None, ("horiz", "lev")),
    )
    out_specs = P(None, None, ("horiz", "lev"))
    return jax.shard_map(local, mesh=mesh, in_specs=in_specs, out_specs=out_specs, check_vma=False)
```

```python
import jax
import jax.numpy as jnp
from jax import lax
from jax.experimental import pallas as pl
from jax.experimental.pallas import tpu as pltpu
from jax.sharding import PartitionSpec as P

SUB = 8
LANES = 128


def shifted(block, axis, distance):
    devices = range(lax.axis_size(axis))
    route = [((i - distance) % len(devices), i) for i in devices]
    return lax.ppermute(block, axis, route)


def select_cells(tile, wanted):
    cell_ids = jnp.arange(tile.shape[1], dtype=jnp.int32)[:, None]
    picker = (cell_ids == wanted[None, :]).astype(jnp.bfloat16)
    return jnp.dot(tile, picker, preferred_element_type=jnp.float32).astype(jnp.bfloat16)


def choose(values, bits):
    for bit in bits:
        pairs = [
            jnp.where(bit, values[i + 1], values[i]) if i + 1 < len(values) else values[i]
            for i in range(0, len(values), 2)
        ]
        values = pairs
    return values[0]


def interpolate_body(lower_ref, upper_ref, fraction_ref, *refs):
    sources, out_ref, held_ref = refs[:-2], refs[-2], refs[-1]
    fields, levels_out, width = out_ref.shape
    slab = sources[0].shape[0] // fields
    tiles = -(-len(sources) * slab // SUB)
    for place, source in enumerate(sources):
        rows = source[...].astype(jnp.float32)
        for f in range(fields):
            held_ref[f, place * slab : (place + 1) * slab, :] = rows[f * slab : (f + 1) * slab]
    digits = max(1, (tiles - 1).bit_length())
    step = 2 * SUB

    def load(ref, first, size, cols):
        value = ref[pl.ds(first, size), cols]
        if size < SUB:
            rest = jnp.zeros((SUB - size, LANES), value.dtype)
            value = jnp.concatenate([value, rest], axis=0)
        return value

    def split(row):
        tile = row >> 3
        return row & (SUB - 1), [(tile & (1 << i)) != 0 for i in range(digits)]

    def fetch(values, row):
        index, bits = row
        return choose(
            [jnp.take_along_axis(v, index, axis=0, mode="promise_in_bounds") for v in values], bits
        )

    def band(first, count, col):
        cols = pl.ds(col, LANES)
        halves = []
        for start in range(0, count, SUB):
            size = min(SUB, count - start)
            share = load(fraction_ref, first + start, size, cols)
            below = split(load(lower_ref, first + start, size, cols))
            above = split(load(upper_ref, first + start, size, cols))
            halves.append((below, above, share, 1.0 - share))
        for f in range(fields):
            values = [held_ref[f, k * SUB : (k + 1) * SUB, cols] for k in range(tiles)]
            results = [
                rest * fetch(values, below) + share * fetch(values, above)
                for below, above, share, rest in halves
            ]
            mixed = jnp.concatenate(results, axis=0)[:count]
            out_ref[f, pl.ds(first, count), cols] = mixed.astype(jnp.bfloat16)

    full = levels_out // step

    @pl.loop(0, width // LANES)
    def _(c):
        col = pl.multiple_of(c * LANES, LANES)

        @pl.loop(0, full)
        def _(j):
            band(pl.multiple_of(j * step, step), step, col)

        if levels_out % step:
            band(full * step, levels_out % step, col)


def interpolate(lower, upper, fraction, slabs, fields):
    rows, width = slabs[0].shape
    held = -(-len(slabs) * rows // fields // SUB) * SUB
    vmem = pl.BlockSpec(memory_space=pltpu.VMEM)
    return pl.pallas_call(
        interpolate_body,
        out_shape=jax.ShapeDtypeStruct((fields, lower.shape[0], width), jnp.bfloat16),
        in_specs=[vmem] * (3 + len(slabs)),
        out_specs=vmem,
        scratch_shapes=[pltpu.VMEM((fields, held, width), jnp.float32)],
        name="interpolate",
    )(lower, upper, fraction, *slabs)


def local(source_state, intersection, index_map, blocks, bracket, fraction):
    fields, level_slab, tile_cells = source_state.shape
    stacked = source_state.reshape(fields * level_slab, tile_cells)
    groups = lax.axis_size("horiz")
    block_count = intersection.shape[0]
    depth = (block_count - 1) // 2
    own_group = lax.axis_index("horiz")
    position = (intersection - own_group + depth) % groups
    collected = []
    for offset in range(-depth, depth + 1):
        wanted_group = (own_group + offset) % groups
        matched = intersection == wanted_group
        request = jnp.sum(jnp.where(matched[:, None], index_map, 0), axis=0)
        if offset == 0:
            collected.append(select_cells(stacked, request))
        else:
            incoming = shifted(request, "horiz", offset)
            outgoing = select_cells(stacked, incoming)
            collected.append(shifted(outgoing, "horiz", -offset))
    reach = jnp.repeat(position, index_map.shape[1])[None, :]
    chosen = jnp.zeros((stacked.shape[0], reach.shape[1]), jnp.bfloat16)
    for place, piece in enumerate(collected):
        chosen = jnp.where(reach == place, jnp.concatenate([piece] * block_count, axis=1), chosen)
    weights_flat = blocks.reshape(-1, blocks.shape[2])
    horizontal = jnp.dot(chosen, weights_flat, preferred_element_type=jnp.float32).astype(
        jnp.bfloat16
    )
    shares = lax.axis_size("lev")
    own_share = lax.axis_index("lev")
    width = blocks.shape[2] // shares
    slabs = []
    for distance in range(shares):
        target = (own_share + distance) % shares
        part = lax.dynamic_slice_in_dim(horizontal, target * width, width, axis=1)
        slabs.append(part if distance == 0 else shifted(part, "lev", distance))

    def place(level):
        return (own_share - level // level_slab) % shares * level_slab + level % level_slab

    return interpolate(place(bracket), place(bracket + 1), fraction, slabs, fields)


def solution(mesh):
    in_specs = (
        P(None, "lev", "horiz"),
        P("horiz"),
        P("horiz", None),
        P("horiz", None, None),
        P(None, ("horiz", "lev")),
        P(None, ("horiz", "lev")),
    )
    out_specs = P(None, None, ("horiz", "lev"))
    return jax.shard_map(local, mesh=mesh, in_specs=in_specs, out_specs=out_specs, check_vma=False)
```

```python
import jax
import jax.numpy as jnp
from jax import lax
from jax.experimental import pallas as pl
from jax.experimental.pallas import tpu as pltpu
from jax.sharding import PartitionSpec as P

SUB = 8
LANES = 128


def shifted(block, axis, distance):
    devices = range(lax.axis_size(axis))
    route = [((i - distance) % len(devices), i) for i in devices]
    return lax.ppermute(block, axis, route)


def select_cells(tile, wanted):
    cell_ids = jnp.arange(tile.shape[1], dtype=jnp.int32)[:, None]
    picker = (cell_ids == wanted[None, :]).astype(jnp.bfloat16)
    return jnp.dot(tile, picker, preferred_element_type=jnp.float32).astype(jnp.bfloat16)


def choose(values, bits):
    for bit in bits:
        pairs = [
            jnp.where(bit, values[i + 1], values[i]) if i + 1 < len(values) else values[i]
            for i in range(0, len(values), 2)
        ]
        values = pairs
    return values[0]


def interpolate_body(lower_ref, upper_ref, fraction_ref, *refs):
    sources, out_ref, held_ref = refs[:-2], refs[-2], refs[-1]
    fields, levels_out, width = out_ref.shape
    slab = sources[0].shape[0] // fields
    tiles = -(-len(sources) * slab // SUB)
    for place, source in enumerate(sources):
        rows = source[...].astype(jnp.float32)
        for f in range(fields):
            held_ref[f, place * slab : (place + 1) * slab, :] = rows[f * slab : (f + 1) * slab]
    digits = max(1, (tiles - 1).bit_length())
    step = 2 * SUB

    def load(ref, first, size, cols):
        value = ref[pl.ds(first, size), cols]
        if size < SUB:
            rest = jnp.zeros((SUB - size, LANES), value.dtype)
            value = jnp.concatenate([value, rest], axis=0)
        return value

    def split(row):
        tile = row >> 3
        return row & (SUB - 1), [(tile & (1 << i)) != 0 for i in range(digits)]

    def fetch(values, row):
        index, bits = row
        return choose(
            [jnp.take_along_axis(v, index, axis=0, mode="promise_in_bounds") for v in values], bits
        )

    def band(first, count, col):
        cols = pl.ds(col, LANES)
        halves = []
        for start in range(0, count, SUB):
            size = min(SUB, count - start)
            share = load(fraction_ref, first + start, size, cols)
            below = split(load(lower_ref, first + start, size, cols))
            above = split(load(upper_ref, first + start, size, cols))
            halves.append((below, above, share, 1.0 - share))
        for f in range(fields):
            values = [held_ref[f, k * SUB : (k + 1) * SUB, cols] for k in range(tiles)]
            results = [
                rest * fetch(values, below) + share * fetch(values, above)
                for below, above, share, rest in halves
            ]
            mixed = jnp.concatenate(results, axis=0)[:count]
            out_ref[f, pl.ds(first, count), cols] = mixed.astype(jnp.bfloat16)

    full = levels_out // step

    @pl.loop(0, width // LANES)
    def _(c):
        col = pl.multiple_of(c * LANES, LANES)

        @pl.loop(0, full)
        def _(j):
            band(pl.multiple_of(j * step, step), step, col)

        if levels_out % step:
            band(full * step, levels_out % step, col)


def interpolate(lower, upper, fraction, slabs, fields):
    rows, width = slabs[0].shape
    held = -(-len(slabs) * rows // fields // SUB) * SUB
    vmem = pl.BlockSpec(memory_space=pltpu.VMEM)
    return pl.pallas_call(
        interpolate_body,
        out_shape=jax.ShapeDtypeStruct((fields, lower.shape[0], width), jnp.bfloat16),
        in_specs=[vmem] * (3 + len(slabs)),
        out_specs=vmem,
        scratch_shapes=[pltpu.VMEM((fields, held, width), jnp.float32)],
        name="interpolate",
    )(lower, upper, fraction, *slabs)


def local(source_state, intersection, index_map, blocks, bracket, fraction):
    fields, level_slab, tile_cells = source_state.shape
    stacked = source_state.reshape(fields * level_slab, tile_cells)
    groups = lax.axis_size("horiz")
    block_count = intersection.shape[0]
    depth = (block_count - 1) // 2
    own_group = lax.axis_index("horiz")
    position = (intersection - own_group + depth) % groups
    offsets = range(-depth, depth + 1)
    requests = {}
    for offset in offsets:
        matched = intersection == (own_group + offset) % groups
        requests[offset] = jnp.sum(jnp.where(matched[:, None], index_map, 0), axis=0)
    away = [offset for offset in offsets if offset != 0]
    arrived = {offset: shifted(requests[offset], "horiz", offset) for offset in away}
    parts = {}
    for offset in away:
        outgoing = select_cells(stacked, arrived[offset])
        parts[offset] = shifted(outgoing, "horiz", -offset)
    held, requests[0] = lax.optimization_barrier((parts[away[-2]], requests[0]))
    parts[away[-2]] = held
    parts[0] = select_cells(stacked, requests[0])
    collected = [parts[offset] for offset in offsets]
    reach = jnp.repeat(position, index_map.shape[1])[None, :]
    chosen = jnp.zeros((stacked.shape[0], reach.shape[1]), jnp.bfloat16)
    for place, piece in enumerate(collected):
        chosen = jnp.where(reach == place, jnp.concatenate([piece] * block_count, axis=1), chosen)
    weights_flat = blocks.reshape(-1, blocks.shape[2])
    chosen, bracket = lax.optimization_barrier((chosen, bracket))
    shares = lax.axis_size("lev")
    own_share = lax.axis_index("lev")
    width = blocks.shape[2] // shares
    slabs = [None] * shares
    for distance in [shares // 2] + [d for d in range(1, shares) if d != shares // 2] + [0]:
        target = (own_share + distance) % shares
        columns = lax.dynamic_slice_in_dim(weights_flat, target * width, width, axis=1)
        part = jnp.dot(chosen, columns, preferred_element_type=jnp.float32).astype(jnp.bfloat16)
        slabs[distance] = part if distance == 0 else shifted(part, "lev", distance)

    def place(level):
        return (own_share - level // level_slab) % shares * level_slab + level % level_slab

    return interpolate(place(bracket), place(bracket + 1), fraction, slabs, fields)


def solution(mesh):
    in_specs = (
        P(None, "lev", "horiz"),
        P("horiz"),
        P("horiz", None),
        P("horiz", None, None),
        P(None, ("horiz", "lev")),
        P(None, ("horiz", "lev")),
    )
    out_specs = P(None, None, ("horiz", "lev"))
    return jax.shard_map(local, mesh=mesh, in_specs=in_specs, out_specs=out_specs, check_vma=False)
```
